256 devices in a mesh: grp: 8 (over z), bis: 32 (over x, y, core).
Axes of the slice: x: 4, y: 4, z: 8, core: 2. Of those that a mesh axis runs over, the one named last changes fastest.
Arguments:
- state: float32 [5, 32768, 512], P(None, ('grp', 'bis')), may hold values from -0.75 to 2, as said below
- order: int32 [256, 32], P(('grp', 'bis')), may hold values from 0 to 31, each once within a row
- sweep: float32 [32768, 512], P(('grp', 'bis')), may hold values from 0.1 to 0.45
- owner: int32 [8192, 1], P(('grp', 'bis')), may hold values from 0 to 31; in each aligned block of 32 rows (0 to 31, 32 to 63, ...) at most 2 rows name the same one
- slot_target: int32 [8192], P(('grp', 'bis')), may hold values from 0 to 31
Outputs:
- mass_out: float32 [32768, 512], P(('grp', 'bis'))
- energy_out: float32 [32768, 512], P(('grp', 'bis'))
- velocity: float32 [2, 32768, 512], P(None, ('grp', 'bis'))
The draws below stay inside these ranges and needn't reach their ends.
Inputs may be any that keep to these rules, and one draw needn't show every extreme that they name: `state`: velocities up to 0.75 in size, densities and energies from 1 to 2, adiabatic indices from 1.3 to 1.7. `order`: each row of a device is a permutation. Among the row blocks of one device no owner is named more than 2 times, a bound that some block reaches.
All inputs are finite; a program needn't handle non-finite values.
Results may differ from the reference program's by a relative error of at most 0.00016.
Values sent between devices are 32-bit elements; how exact they have to be, the bound alone decides.
A program may use at most 64 MiB of HBM per device.

```python
import math
import jax
import jax.numpy as jnp
import numpy as np

W = 512
BR = 4
STEPS = 2
CAP = 2
NBLK = 32
ROWS = 32768
BLOCKS = 8192
N_GRP = 8
N_BIS = 32


def draw_state(key, part):
    keys = jax.random.split(key, 5)
    shape = (ROWS, W)
    rho = jax.random.uniform(keys[0], shape, jnp.float32, 1.0, 2.0)
    ene = 1.0 + jax.random.uniform(keys[1], shape, jnp.float32, 0.0, 1.0)
    velu = 0.3 * jnp.clip(jax.random.normal(keys[2], shape, jnp.float32), -2.5, 2.5)
    velv = 0.3 * jnp.clip(jax.random.normal(keys[3], shape, jnp.float32), -2.5, 2.5)
    gam = jax.random.uniform(keys[4], shape, jnp.float32, 1.3, 1.7)
    return jnp.stack([rho, ene, velu, velv, gam]).astype(jnp.float32)


def touch_ends(values, own_key, smallest, top_value):
    longest = values.shape.index(max(values.shape))
    spots = []
    for shift in (0, 1):
        where = [jax.random.randint(jax.random.fold_in(own_key, axis), (), 0, length) for axis, length in enumerate(values.shape)]
        where[longest] = (where[longest] + shift) % values.shape[longest]
        spots.append(tuple(where))
    return values.at[spots[0]].set(smallest).at[spots[1]].set(top_value)


def block_levels(rng, extent, cuts, least, largest):
    level, own = 1.0, jax.random.fold_in(rng, 6)
    for axis_at, blocks in cuts:
        draws = jnp.exp(jax.random.uniform(jax.random.fold_in(own, axis_at), (blocks,), jnp.float32, least / len(cuts), largest / len(cuts)))
        level = level * jnp.repeat(draws, extent[axis_at] // blocks).reshape([-1 if axis == axis_at else 1 for axis in range(len(extent))])
    return level


def assign_block(key, own, number, rows, number_of, top, most, slope):
    sequence = jax.random.permutation(key, number_of)
    packed, usual = portions_of(number_of, rows * top, most, slope, True), portions_of(number_of, rows * top, most, slope, False)
    places = jnp.arange(number_of)

    def named(tallies, turn):
        used = int((tallies > 0).sum())
        fixed = max(1, used // 4)
        moved = fixed + (places - fixed + turn * (used - fixed)) % max(1, number_of - fixed)
        return jnp.zeros((number_of,), jnp.int32).at[sequence[jnp.where(places < fixed, places, moved)]].set(jnp.asarray(tallies, jnp.int32))

    tallies = jnp.where(number % 4 == 0, named(packed, number // 4), named(usual, number - number // 4 - 1))
    mixed = jax.random.permutation(jax.random.fold_in(own, 3), number_of)
    donor, sink = mixed[0:number_of // 2 * 2:2], mixed[1:number_of // 2 * 2:2]
    slack = jnp.minimum(tallies[donor] - 1, most - tallies[sink]) // 2
    slack = jnp.where((donor == sequence[0]) | (sink == sequence[0]) | (tallies[sink] == 0), 0, jnp.maximum(slack, 0))
    moved = jax.random.randint(jax.random.fold_in(own, 4), (number_of // 2,), 0, 1 << 20) % (slack + 1)
    tallies = tallies.at[donor].add(-moved).at[sink].add(moved)
    members = jnp.searchsorted(jnp.cumsum(tallies), jnp.arange(rows * top), side="right").astype(jnp.int32)
    listing = members.reshape(top, rows).T
    listing = listing[jax.random.permutation(jax.random.fold_in(own, 1), rows)]
    turn = jax.random.randint(jax.random.fold_in(own, 2), (rows, 1), 0, top)
    return jnp.take_along_axis(listing, (jnp.arange(top)[None, :] + turn) % top, axis=1)


def portions_of(number_of, total, limit, slope, full):
    loads = [(1 << 20) // math.isqrt(standing ** slope) + 1 for standing in range(1, number_of + 1)]
    largest = limit if full else min(limit, max(-(-total // number_of), total * loads[0] // sum(loads)))
    least = 1 if total - largest >= number_of - 1 else 0
    given, surplus = [largest] + [least] * (number_of - 1), total - largest - least * (number_of - 1)
    while surplus > 0:
        movable = [i for i in range(1, number_of) if given[i] < largest] or [i for i in range(1, number_of) if given[i] < limit]
        whole, budget = sum([loads[i] for i in movable]), surplus
        for i in movable:
            more = min(limit - given[i], max(1, budget * loads[i] // whole), surplus)
            given[i] = given[i] + more
            surplus = surplus - more
    return np.array(given)


def setup_inputs(seed: int = 0) -> dict:
    arg_keys = jax.random.split(jax.random.key(seed), 6)
    state = draw_state(jax.random.fold_in(arg_keys[5], 71), 0)
    order = jax.vmap(lambda own: jax.random.permutation(own, N_BIS))(jax.random.split(arg_keys[1], (N_GRP * N_BIS))).reshape((N_GRP * N_BIS, N_BIS)).astype(jnp.int32)
    sweep = jnp.clip(0.1 + 0.35 * jax.random.uniform(arg_keys[2], (ROWS, W), jnp.float32) ** block_levels(arg_keys[2], (ROWS, W), ((0, 256),), -0.2, 0.2), 0.1, 0.45)
    owner_keys = jax.random.split(jax.random.fold_in(arg_keys[3], 1), BLOCKS // NBLK)
    owner_turns = jax.random.permutation(jax.random.fold_in(arg_keys[3], 3), BLOCKS // NBLK)
    owner = jax.vmap(lambda own, number: assign_block(jax.random.fold_in(arg_keys[3], 2), own, number, NBLK, N_BIS, 1, CAP, 2))(owner_keys, owner_turns).reshape((BLOCKS, 1))
    slot_target = touch_ends(jax.random.randint(arg_keys[4], (BLOCKS,), 0, NBLK), jax.random.fold_in(arg_keys[4], 1), 0, NBLK - 1).astype(jnp.int32)
    return {"state": state, "order": order, "sweep": sweep, "owner": owner, "slot_target": slot_target}


STEP_DT = 0.15


def advance(fields, volume, valid):
    rho = fields[0]
    ene = fields[1]
    velu = fields[2]
    velv = fields[3]
    gam = fields[4]
    press = (gam - 1.0) * rho * ene
    wide_p = jnp.pad(press[1:-1], ((0, 0), (1, 1)))
    wide_v = jnp.pad(velv[1:-1], ((0, 0), (1, 1)))
    grad_x = 0.5 * (press[2:] - press[:-2])
    grad_y = 0.5 * (wide_p[:, 2:] - wide_p[:, :-2])
    spread = 0.5 * (velu[2:] - velu[:-2] + wide_v[:, 2:] - wide_v[:, :-2])
    dens = jnp.where(valid, rho[1:-1], 1.0)
    growth = 1.0 + STEP_DT * spread
    center_g = gam[1:-1]
    updated = jnp.stack([
        dens / growth,
        ene[1:-1] * (1.0 - STEP_DT * (center_g - 1.0) * spread),
        velu[1:-1] - STEP_DT * grad_x / dens,
        velv[1:-1] - STEP_DT * grad_y / dens,
        center_g,
    ])
    updated = jnp.where(valid[None], updated, 0.0)
    return updated, volume * growth


def reference(state, order, sweep, owner, slot_target):
    blocks = state.reshape(5, N_GRP, N_BIS, NBLK, BR, W)
    order_g = order.reshape(N_GRP, N_BIS, N_BIS)
    picked = jnp.take_along_axis(blocks, order_g[None, :, :, :, None, None], axis=3)
    fields = jnp.transpose(picked, (0, 1, 3, 2, 4, 5)).reshape(5, ROWS, W)
    volume = jnp.ones((ROWS, W), jnp.float32)
    valid = jnp.ones((ROWS, 1), bool)
    for step in range(STEPS):
        padded = jnp.pad(fields, ((0, 0), (1, 1), (0, 0)))
        fields, volume = advance(padded, volume, valid)
    mass = fields[0] * volume
    heat = mass * fields[1]
    frac = sweep * volume / (1.0 + volume)
    amounts = jnp.stack([mass, heat])
    stay = ((1.0 - frac) * amounts).reshape(2, ROWS // BR, BR, W)
    leave = jnp.roll((frac * amounts).reshape(2, ROWS // BR, BR, W), 1, axis=2)
    partial_value = (stay + leave).reshape(2, N_GRP, N_BIS * NBLK, BR * W)
    partial_value = jnp.transpose(partial_value, (1, 2, 0, 3))
    labels = (owner[:, 0].reshape(N_GRP, N_BIS * NBLK) * NBLK + slot_target.reshape(N_GRP, N_BIS * NBLK)).astype(jnp.int32)

    def one_group(data, seg):
        return jax.ops.segment_sum(data, seg, num_segments=N_BIS * NBLK)

    summed = jax.vmap(one_group)(partial_value, labels)
    summed = jnp.transpose(summed, (2, 0, 1, 3)).reshape(2, ROWS, W)
    return summed[0], summed[1], fields[2:4]
```

```python
import functools

import jax
import jax.numpy as jnp
from jax import lax
from jax.experimental import pallas as pl
from jax.experimental.pallas import tpu as pltpu
from jax.sharding import PartitionSpec as P

DT = 0.15
NB = 32
NG = 8
W = 512
LANE = 128
SPLIT = W // LANE
BLK = 4 * SPLIT
BASE = 16
EXT = BASE + NB * BLK + 16
MESH = pl.DeviceIdType.MESH
STRIDE = 11


def neighbour(me, k):
    j = lax.rem(k * STRIDE, NB)
    x, y, c = me // 8, lax.rem(me // 2, 4), lax.rem(me, 2)
    dx, dy, dc = j // 8, lax.rem(j // 2, 4), lax.rem(j, 2)
    return lax.rem(x + dx, 4) * 8 + lax.rem(y + dy, 4) * 2 + lax.rem(c + dc, 2)


def rows_of(block):
    return pl.multiple_of(BASE + block * BLK, 8)


def step_block(at, size, rho_ref, ene_ref, velu_ref, velv_ref, gam, press_ref):
    lane = lax.broadcasted_iota(jnp.int32, (size, LANE), 1)
    piece = lax.rem(lax.broadcasted_iota(jnp.int32, (size, LANE), 0), SPLIT)

    def ld(ref, off):
        return ref[pl.ds(at + off, size), :]

    def columns(ref):
        here = ld(ref, 0)
        before = jnp.where(piece == 0, 0.0, ld(ref, -1))
        after = jnp.where(piece == SPLIT - 1, 0.0, ld(ref, 1))
        left = pltpu.roll(jnp.where(lane == LANE - 1, before, here), 1, 1)
        right = pltpu.roll(jnp.where(lane == 0, after, here), LANE - 1, 1)
        return right - left

    dens = ld(rho_ref, 0)
    ene = ld(ene_ref, 0)
    grad_x = 0.5 * (ld(press_ref, SPLIT) - ld(press_ref, -SPLIT))
    grad_y = 0.5 * columns(press_ref)
    spread = 0.5 * (ld(velu_ref, SPLIT) - ld(velu_ref, -SPLIT) + columns(velv_ref))
    growth = 1.0 + DT * spread
    inverse = 1.0 / dens
    return (
        dens / growth,
        ene * (1.0 - DT * (gam - 1.0) * spread),
        ld(velu_ref, 0) - DT * grad_x * inverse,
        ld(velv_ref, 0) - DT * grad_y * inverse,
        growth,
    )


def main_kernel(
    order_ref, plan_ref, state_ref, meta_ref, sweep_ref,
    arr_ref, got_ref, vel_ref,
    xv, lin, snd, ext, press, one, snd2, part, swl, vel,
    in_sem, s1, r1, sm, rm, sh, rh, s2, r2, out_sem,
):
    grp = lax.axis_index("grp")
    me = lax.axis_index("bis")
    whole = grp * NB + me
    has_low = whole > 0
    has_high = whole < NG * NB - 1
    low = (grp - (me == 0).astype(jnp.int32), lax.rem(me + NB - 1, NB))
    high = (grp + (me == NB - 1).astype(jnp.int32), lax.rem(me + 1, NB))
    far_low = jnp.logical_and(me == 0, has_low)
    far_high = jnp.logical_and(me == NB - 1, has_high)

    barrier = pltpu.get_barrier_semaphore()

    loads = [
        pltpu.make_async_copy(state_ref.at[f], xv.at[f], in_sem.at[f]) for f in range(5)
    ]
    for load in loads:
        load.start()

    def greet(k, carry):
        pl.semaphore_signal(
            barrier, inc=1, device_id=(grp, neighbour(me, k)), device_id_type=MESH
        )
        return carry

    lax.fori_loop(1, NB, greet, 0)

    @pl.when(far_low)
    def _():
        pl.semaphore_signal(barrier, inc=1, device_id=low, device_id_type=MESH)

    @pl.when(far_high)
    def _():
        pl.semaphore_signal(barrier, inc=1, device_id=high, device_id_type=MESH)

    flat = lin.reshape(5, NB * BLK, LANE)
    for f in range(5):
        loads[f].wait()
        for i in range(16):
            for c in range(SPLIT):
                flat[f, pl.ds(i * 8 * SPLIT + c, 8, stride=SPLIT), :] = xv[
                    f, i * 8 : i * 8 + 8, c * LANE : c * LANE + LANE
                ]

    def picked(d):
        return lin[:, order_ref[0, d]]

    def pack(k):
        d = neighbour(me, k)
        snd[d] = picked(d)

    pl.semaphore_wait(
        barrier, NB - 1 + far_low.astype(jnp.int32) + far_high.astype(jnp.int32)
    )

    def move(d, source):
        return pltpu.make_async_remote_copy(
            src_ref=snd.at[d],
            dst_ref=ext.at[:, pl.ds(rows_of(source), BLK), :],
            send_sem=s1.at[d],
            recv_sem=r1.at[source],
            device_id=(grp, d),
            device_id_type=MESH,
        )

    def tell(d, source):
        return pltpu.make_async_remote_copy(
            src_ref=meta_ref,
            dst_ref=got_ref.at[source],
            send_sem=sm.at[d],
            recv_sem=rm.at[source],
            device_id=(grp, d),
            device_id_type=MESH,
        )

    pack(1)

    def send(k, carry):
        @pl.when(k < NB - 1)
        def _():
            pack(k + 1)

        move(neighbour(me, k), me).start()
        return carry

    lax.fori_loop(1, NB, send, 0)

    def send_meta(k, carry):
        tell(neighbour(me, k), me).start()
        return carry

    lax.fori_loop(1, NB, send_meta, 0)
    own_meta = pltpu.make_async_copy(meta_ref, got_ref.at[me], out_sem.at[2])
    own_meta.start()

    ext[:, pl.ds(rows_of(me), BLK), :] = picked(me)
    zero = jnp.zeros((8, LANE), jnp.float32)
    for f in range(5):
        ext[f, 0:8, :] = zero
        ext[f, EXT - 8 : EXT, :] = zero

    @pl.when(jnp.logical_not(has_low))
    def _():
        for f in range(5):
            ext[f, 8:16, :] = zero

    @pl.when(jnp.logical_not(has_high))
    def _():
        for f in range(5):
            ext[f, EXT - 16 : EXT - 8, :] = zero

    press[0, 0:8, :] = zero
    press[0, EXT - 8 : EXT, :] = zero
    for i in range(16):
        for c in range(SPLIT):
            swl[pl.ds(i * 8 * SPLIT + c, 8, stride=SPLIT), :] = sweep_ref[
                i * 8 : i * 8 + 8, c * LANE : c * LANE + LANE
            ]

    def pressure(at, size):
        rows = pl.ds(at, size)
        press[0, rows, :] = (ext[4, rows, :] - 1.0) * ext[0, rows, :] * ext[1, rows, :]

    pressure(rows_of(me), BLK)

    def arrive(k, carry):
        source = neighbour(me, k)
        move(source, source).wait_recv()
        pressure(rows_of(source), BLK)
        return carry

    lax.fori_loop(1, NB, arrive, 0)

    up = pltpu.make_async_remote_copy(
        src_ref=ext.at[:, pl.ds(EXT - 24, 8), :],
        dst_ref=ext.at[:, pl.ds(8, 8), :],
        send_sem=sh.at[0],
        recv_sem=rh.at[0],
        device_id=high,
        device_id_type=MESH,
    )
    down = pltpu.make_async_remote_copy(
        src_ref=ext.at[:, pl.ds(BASE, 8), :],
        dst_ref=ext.at[:, pl.ds(EXT - 16, 8), :],
        send_sem=sh.at[1],
        recv_sem=rh.at[1],
        device_id=low,
        device_id_type=MESH,
    )

    @pl.when(has_high)
    def _():
        up.start()

    @pl.when(has_low)
    def _():
        down.start()

    def first(at, size, keep=None):
        gam = ext[4, pl.ds(at, size), :]
        rho, ene, velu, velv, growth = step_block(
            at, size, ext.at[0], ext.at[1], ext.at[2], ext.at[3], gam, press.at[0]
        )
        pre = (gam - 1.0) * rho * ene
        if keep is not None:
            velu = jnp.where(keep, velu, 0.0)
            pre = jnp.where(keep, pre, 0.0)
        rows = pl.ds(at, size)
        one[0, rows, :] = rho
        one[1, rows, :] = ene
        one[2, rows, :] = velu
        one[3, rows, :] = velv
        one[4, rows, :] = growth
        press[1, rows, :] = pre

    def second(block):
        at = rows_of(block)
        gam = ext[4, pl.ds(at, BLK), :]
        rho, ene, velu, velv, growth = step_block(
            at, BLK, one.at[0], one.at[1], one.at[2], one.at[3], gam, press.at[1]
        )
        volume = one[4, pl.ds(at, BLK), :] * growth
        here = pl.multiple_of(block * BLK, BLK)
        vel[0, pl.ds(here, BLK), :] = velu
        vel[1, pl.ds(here, BLK), :] = velv
        mass = rho * volume
        heat = mass * ene
        frac = swl[pl.ds(here, BLK), :] * volume / (1.0 + volume)
        part[block, 0] = (1.0 - frac) * mass + pltpu.roll(frac * mass, SPLIT, 0)
        part[block, 1] = (1.0 - frac) * heat + pltpu.roll(frac * heat, SPLIT, 0)

    def first_loop(b, carry):
        first(rows_of(b), BLK)
        return carry

    def second_loop(b, carry):
        second(b)
        return carry

    lax.fori_loop(1, NB - 1, first_loop, 0)
    lax.fori_loop(2, NB - 2, second_loop, 0)

    @pl.when(has_low)
    def _():
        up.wait_recv()

    @pl.when(has_high)
    def _():
        down.wait_recv()

    pressure(8, 8)
    pressure(EXT - 16, 8)
    first(8, 8, has_low)
    first(EXT - 16, 8, has_high)

    def edge_first(j, carry):
        first(rows_of(j * (NB - 1)), BLK)
        return carry

    lax.fori_loop(0, 2, edge_first, 0)

    def edge_second(j, carry):
        second(j + (j // 2) * (NB - 4))
        return carry

    lax.fori_loop(0, 4, edge_second, 0)

    vel_out = pltpu.make_async_copy(vel, vel_ref, out_sem.at[0])

    def share(d, source):
        return pltpu.make_async_remote_copy(
            src_ref=snd2.at[d],
            dst_ref=arr_ref.at[source],
            send_sem=s2.at[d],
            recv_sem=r2.at[source],
            device_id=(grp, d),
            device_id_type=MESH,
        )

    def pack2(d):
        snd2[d, 0] = part[plan_ref[0, 64 + d]]
        snd2[d, 1] = part[plan_ref[0, 96 + d]]

    pack2(neighbour(me, 1))

    def send2(k, carry):
        @pl.when(k < NB - 1)
        def _():
            pack2(neighbour(me, k + 1))

        share(neighbour(me, k), me).start()
        return carry

    lax.fori_loop(1, NB, send2, 0)
    pack2(me)
    vel_out.start()
    own = pltpu.make_async_copy(snd2.at[me], arr_ref.at[me], out_sem.at[1])
    own.start()

    def finish(k, carry):
        d = neighbour(me, k)
        move(d, me).wait_send()
        tell(d, me).wait_send()
        tell(d, d).wait_recv()
        return carry

    lax.fori_loop(1, NB, finish, 0)

    @pl.when(has_high)
    def _():
        up.wait_send()

    @pl.when(has_low)
    def _():
        down.wait_send()

    def finish2(k, carry):
        d = neighbour(me, k)
        share(d, d).wait_recv()
        share(d, me).wait_send()
        return carry

    lax.fori_loop(1, NB, finish2, 0)
    own_meta.wait()
    vel_out.wait()
    own.wait()


def last_kernel(got_ref, arr_ref, vel_ref, mass_ref, heat_ref, velo_ref, acc):
    me = lax.axis_index("bis")
    for q in range(2):
        acc[q] = jnp.zeros(acc.shape[1:], jnp.float32)

    def add(source, carry):
        for k in range(2):
            at = pl.multiple_of(got_ref[source, 0, k * NB + me] * BLK, BLK)
            for q in range(2):
                acc[q, pl.ds(at, BLK), :] += arr_ref[source, k, q]
        return carry

    lax.fori_loop(0, NB, add, 0)
    for i in range(16):
        for c in range(SPLIT):
            rows = pl.ds(i * 8 * SPLIT + c, 8, stride=SPLIT)
            put = (slice(i * 8, i * 8 + 8), slice(c * LANE, c * LANE + LANE))
            mass_ref[put] = acc[0, rows, :]
            heat_ref[put] = acc[1, rows, :]
            velo_ref[(0,) + put] = vel_ref[0, rows, :]
            velo_ref[(1,) + put] = vel_ref[1, rows, :]


def shards(state, order, sweep, owner, slot_target):
    f32 = jnp.float32
    index = jnp.arange(NB, dtype=jnp.int32)
    code = index * NB + slot_target
    hit = owner == index[None, :]
    low = jnp.min(jnp.where(hit, code[:, None], NB * NB), axis=0)
    high = jnp.max(jnp.where(hit, code[:, None], -1), axis=0)
    plan = jnp.concatenate(
        [
            jnp.where(low < NB * NB, low % NB, NB),
            jnp.where(high > low, high % NB, NB),
            jnp.minimum(low // NB, NB - 1),
            jnp.maximum(high, 0) // NB,
        ]
    ).reshape(1, 4 * NB)
    any_ = pl.BlockSpec(memory_space=pl.ANY)
    vmem = pl.BlockSpec(memory_space=pltpu.VMEM)
    smem = pl.BlockSpec(memory_space=pltpu.SMEM)
    dma = pltpu.SemaphoreType.DMA
    arrived, got, vel = pl.pallas_call(
        main_kernel,
        name="step",
        out_shape=(
            jax.ShapeDtypeStruct((NB, 2, 2, BLK, LANE), f32),
            jax.ShapeDtypeStruct((NB, 1, LANE), jnp.int32),
            jax.ShapeDtypeStruct((2, NB * BLK, LANE), f32),
        ),
        in_specs=[smem, smem, any_, any_, vmem],
        out_specs=(any_, any_, any_),
        scratch_shapes=[
            pltpu.VMEM((5, 128, W), f32),
            pltpu.VMEM((5, NB, BLK, LANE), f32),
            pltpu.VMEM((NB, 5, BLK, LANE), f32),
            pltpu.VMEM((5, EXT, LANE), f32),
            pltpu.VMEM((2, EXT, LANE), f32),
            pltpu.VMEM((5, EXT, LANE), f32),
            pltpu.VMEM((NB, 2, 2, BLK, LANE), f32),
            pltpu.VMEM((NB, 2, BLK, LANE), f32),
            pltpu.VMEM((NB * BLK, LANE), f32),
            pltpu.VMEM((2, NB * BLK, LANE), f32),
            dma((5,)),
            dma((NB,)), dma((NB,)),
            dma((NB,)), dma((NB,)),
            dma((2,)), dma((2,)),
            dma((NB,)), dma((NB,)),
            dma((3,)),
        ],
        compiler_params=pltpu.CompilerParams(collective_id=0, has_side_effects=True),
    )(order, plan, state, plan, sweep)
    shape = jax.ShapeDtypeStruct((128, W), f32)
    return pl.pallas_call(
        last_kernel,
        name="gather",
        out_shape=(shape, shape, jax.ShapeDtypeStruct((2, 128, W), f32)),
        in_specs=[smem, vmem, vmem],
        out_specs=(vmem, vmem, vmem),
        scratch_shapes=[pltpu.VMEM((2, (NB + 1) * BLK, LANE), f32)],
    )(got, arrived, vel)


def solution(mesh):
    rows = P(("grp", "bis"), None)
    return jax.shard_map(
        shards,
        mesh=mesh,
        in_specs=(P(None, ("grp", "bis"), None), rows, rows, rows, P(("grp", "bis"))),
        out_specs=(rows, rows, P(None, ("grp", "bis"), None)),
        check_vma=False,
    )
```

```python
import jax
import jax.numpy as jnp
from jax import lax
from jax.experimental import pallas as pl
from jax.experimental.pallas import tpu as pltpu
from jax.sharding import PartitionSpec as P

DT = 0.15
NB = 32
NG = 8
W = 512
ROWS = 128
BR = 4
LANE = 128
PIECES = W // LANE
EARLY = 3
LATE = PIECES - EARLY
TOP = 16
EXT = TOP + ROWS + 16
MESH = pl.DeviceIdType.MESH
STRIDE = 13
HOLD = 16
F32 = jnp.float32


def neighbour(me, k):
    j = lax.rem(k * STRIDE, NB)
    x, y, c = me // 8, lax.rem(me // 2, 4), lax.rem(me, 2)
    dx, dy, dc = j // 8, lax.rem(j // 2, 4), lax.rem(j, 2)
    return lax.rem(x + dx, 4) * 8 + lax.rem(y + dy, 4) * 2 + lax.rem(c + dc, 2)


def lane_mask(size, lane):
    return lax.broadcasted_iota(jnp.int32, (size, LANE), 1) == lane


def advance(piece, at, size, fields, press, closed):
    def ld(ref, off=0, where=piece):
        return ref[where, pl.ds(at + off, size), :]

    def columns(ref):
        here = ld(ref)
        before = ld(ref, 0, piece - 1) if piece > 0 else 0.0
        after = ld(ref, 0, piece + 1) if piece + 1 < PIECES and not closed else 0.0
        left = pltpu.roll(jnp.where(lane_mask(size, LANE - 1), before, here), 1, 1)
        right = pltpu.roll(jnp.where(lane_mask(size, 0), after, here), LANE - 1, 1)
        return right - left

    rho, ene, velu, velv, gam = fields
    dens = ld(rho)
    grad_x = 0.5 * (ld(press, 1) - ld(press, -1))
    grad_y = 0.5 * columns(press)
    spread = 0.5 * (ld(velu, 1) - ld(velu, -1) + columns(velv))
    growth = 1.0 + DT * spread
    inverse = 1.0 / dens
    gamma = ld(gam)
    return (
        dens / growth,
        ld(ene) * (1.0 - DT * (gamma - 1.0) * spread),
        ld(velu) - DT * grad_x * inverse,
        ld(velv) - DT * grad_y * inverse,
        growth,
        gamma,
    )


def main_kernel(
    order_ref, owner_ref, slot_ref, state_ref, sweep_ref,
    arr_a, arr_b, got_ref, vel_ref,
    xv, lin_a, lin_b, snd_a, snd_b, msg_a, msg_b, hal_a, hal_b,
    ext, one, press0, press1, part_a, part_b, out_a, out_b, vel, plan_v, plan_s,
    in_sem, s1a, r1a, s1b, r1b, sm, rm, sh, rh, s2a, r2a, s2b, r2b, loc,
):
    grp = lax.axis_index("grp")
    me = lax.axis_index("bis")
    whole = grp * NB + me
    has_low = whole > 0
    has_high = whole < NG * NB - 1
    first_one = me == 0
    last_one = me == NB - 1
    low = (grp - first_one.astype(jnp.int32), lax.rem(me + NB - 1, NB))
    high = (grp + last_one.astype(jnp.int32), lax.rem(me + 1, NB))
    far_low = jnp.logical_and(first_one, has_low)
    far_high = jnp.logical_and(last_one, has_high)

    loads = [pltpu.make_async_copy(state_ref.at[f], xv.at[f], in_sem.at[f]) for f in range(5)]
    for load in loads:
        load.start()

    barrier = pltpu.get_barrier_semaphore()

    def loop(lo, hi, body):
        def step(k, carry):
            body(k)
            return carry

        lax.fori_loop(lo, hi, step, 0)

    def greet(k):
        pl.semaphore_signal(
            barrier, inc=1, device_id=(grp, neighbour(me, k)), device_id_type=MESH
        )

    loop(1, NB, greet)

    @pl.when(far_low)
    def _():
        pl.semaphore_signal(barrier, inc=1, device_id=low, device_id_type=MESH)

    @pl.when(far_high)
    def _():
        pl.semaphore_signal(barrier, inc=1, device_id=high, device_id_type=MESH)

    row = lax.broadcasted_iota(jnp.int32, (NB, LANE), 0)
    lane = lax.broadcasted_iota(jnp.int32, (NB, LANE), 1)
    same = lax.broadcasted_iota(jnp.int32, (NB, NB), 0) == lax.broadcasted_iota(
        jnp.int32, (NB, NB), 1
    )

    def column(ref):
        spread = jnp.where(same, jnp.broadcast_to(ref[...], (NB, NB)), 0)
        return jnp.sum(spread, axis=1, keepdims=True)

    code = row * NB + column(slot_ref)
    hit = jnp.broadcast_to(column(owner_ref), (NB, LANE)) == lax.rem(lane, NB)
    least = jnp.min(jnp.where(hit, code, NB * NB), axis=0, keepdims=True)
    most = jnp.max(jnp.where(hit, code, -1), axis=0, keepdims=True)
    at_lane = lax.broadcasted_iota(jnp.int32, (1, LANE), 1)
    plan_v[...] = jnp.where(
        at_lane < NB,
        jnp.where(least < NB * NB, least & (NB - 1), NB),
        jnp.where(
            at_lane < 2 * NB,
            jnp.where(most > least, most & (NB - 1), NB),
            jnp.where(
                at_lane < 3 * NB,
                jnp.minimum(least >> 5, NB - 1),
                jnp.maximum(most, 0) >> 5,
            ),
        ),
    )

    for f in range(5):
        loads[f].wait()
        for c in range(PIECES):
            for b in range(NB):
                half = xv[f, b * BR : b * BR + BR, c * LANE : c * LANE + LANE]
                if c < EARLY:
                    lin_a[b, f, c] = half
                else:
                    lin_b[b, f, c - EARLY] = half

    plan_copy = pltpu.make_async_copy(plan_v, plan_s, loc.at[0])
    plan_copy.start()
    pl.semaphore_wait(
        barrier, NB - 1 + far_low.astype(jnp.int32) + far_high.astype(jnp.int32)
    )

    def remote(src, dst, send, recv, d):
        return pltpu.make_async_remote_copy(
            src_ref=src, dst_ref=dst, send_sem=send, recv_sem=recv,
            device_id=(grp, d), device_id_type=MESH,
        )

    def move_a(d, source):
        return remote(snd_a.at[d], msg_a.at[source], s1a.at[d], r1a.at[source], d)

    def move_b(d, source):
        return remote(snd_b.at[d], msg_b.at[source], s1b.at[d], r1b.at[source], d)

    def tell(d, source):
        return remote(plan_v, got_ref.at[source], sm.at[d], rm.at[source], d)

    def share_a(d, source):
        return remote(out_a.at[d], arr_a.at[source], s2a.at[d], r2a.at[source], d)

    def share_b(d, source):
        return remote(out_b.at[d], arr_b.at[source], s2b.at[d], r2b.at[source], d)

    def fill_a(k):
        d = neighbour(me, k)
        snd_a[d] = lin_a[order_ref[0, d]]

    def fill_b(k):
        d = neighbour(me, k)
        snd_b[d] = lin_b[order_ref[0, d]]

    fill_a(1)

    def go_a(k):
        @pl.when(k < NB - 1)
        def _():
            fill_a(k + 1)

        move_a(neighbour(me, k), me).start()

    loop(1, NB, go_a)
    loop(1, NB, fill_b)
    loop(1, NB - HOLD, lambda k: move_b(neighbour(me, k), me).start())
    loop(1, NB, lambda k: tell(neighbour(me, k), me).start())
    own_plan = pltpu.make_async_copy(plan_v, got_ref.at[me], loc.at[1])
    own_plan.start()
    msg_a[me] = lin_a[order_ref[0, me]]
    msg_b[me] = lin_b[order_ref[0, me]]

    zero = jnp.zeros((TOP, LANE), F32)
    for c in range(PIECES):
        for f in range(5):
            ext[f, c, 0:TOP, :] = zero
            ext[f, c, EXT - 16 : EXT, :] = zero
        press0[c, 0:TOP, :] = zero
        press0[c, EXT - 16 : EXT, :] = zero

    def spread_out(values, c, at):
        for f in range(5):
            ext[f, c, pl.ds(at, BR), :] = values[f]
        press0[c, pl.ds(at, BR), :] = (values[4] - 1.0) * values[0] * values[1]

    def unpack(msg, base, count, source):
        for c in range(count):
            spread_out([msg[source, f, c] for f in range(5)], base + c, TOP + source * BR)

    def halo(hal, msg, at):
        up = pltpu.make_async_remote_copy(
            src_ref=msg.at[NB - 1], dst_ref=hal.at[0], send_sem=sh.at[at], recv_sem=rh.at[at],
            device_id=high, device_id_type=MESH,
        )
        down = pltpu.make_async_remote_copy(
            src_ref=msg.at[0], dst_ref=hal.at[1], send_sem=sh.at[at + 1], recv_sem=rh.at[at + 1],
            device_id=low, device_id_type=MESH,
        )
        return up, down

    def pass_on(pair, move):
        up, down = pair

        @pl.when(jnp.logical_not(last_one))
        def _():
            move(NB - 1, NB - 1).wait_recv()

        @pl.when(has_high)
        def _():
            up.start()

        @pl.when(jnp.logical_not(first_one))
        def _():
            move(0, 0).wait_recv()

        @pl.when(has_low)
        def _():
            down.start()

    def collect(move, msg, base, count):
        def one_source(k):
            source = neighbour(me, k)

            @pl.when(jnp.logical_and(source > 0, source < NB - 1))
            def _():
                move(source, source).wait_recv()

            unpack(msg, base, count, source)

        loop(1, NB, one_source)
        unpack(msg, base, count, me)

    def halo_in(pair, hal, base, count):
        up, down = pair

        @pl.when(has_low)
        def _():
            up.wait_recv()
            for c in range(count):
                spread_out([hal[0, f, c] for f in range(5)], base + c, TOP - BR)

        @pl.when(has_high)
        def _():
            down.wait_recv()
            for c in range(count):
                spread_out([hal[1, f, c] for f in range(5)], base + c, TOP + ROWS)

    start = [ext.at[f] for f in range(5)]
    after = [one.at[f] for f in range(4)] + [ext.at[4]]

    def first(pieces, at, size, closed=None, keep=None):
        rows = pl.ds(at, size)
        done = [advance(c, at, size, start, press0, c == closed) for c in pieces]
        for c, (rho, ene, velu, velv, growth, gamma) in zip(pieces, done):
            pre = (gamma - 1.0) * rho * ene
            if keep is not None:
                velu = jnp.where(keep, velu, 0.0)
                pre = jnp.where(keep, pre, 0.0)
            one[0, c, rows, :] = rho
            one[1, c, rows, :] = ene
            one[2, c, rows, :] = velu
            one[3, c, rows, :] = velv
            one[4, c, rows, :] = growth
            press1[c, rows, :] = pre

    def second(pieces, block, size, part):
        mesh_row = pl.multiple_of(block * BR, 8)
        at = pl.multiple_of(TOP + block * BR, 8)
        done = [advance(c, at, size, after, press1, False) for c in pieces]
        head = lax.rem(lax.broadcasted_iota(jnp.int32, (size, LANE), 0), BR) == 0

        def mixed(value, frac):
            away = frac * value
            near = pltpu.roll(away, 1, 0)
            wrap = pltpu.roll(away, size - (BR - 1), 0)
            return (1.0 - frac) * value + jnp.where(head, wrap, near)

        for c, (rho, ene, velu, velv, growth, _) in zip(pieces, done):
            columns = slice(c * LANE, c * LANE + LANE)
            volume = one[4, c, pl.ds(at, size), :] * growth
            vel[0, pl.ds(mesh_row, size), columns] = velu
            vel[1, pl.ds(mesh_row, size), columns] = velv
            mass = rho * volume
            heat = mass * ene
            frac = sweep_ref[pl.ds(mesh_row, size), columns] * volume / (1.0 + volume)
            for q, value in enumerate((mixed(mass, frac), mixed(heat, frac))):
                put = q * 8 + (c % 2) * BR
                for i in range(size // BR):
                    part[block + i, put : put + BR, :] = value[i * BR : i * BR + BR]

    def inner_rows(pieces, closed, results, part):
        loop(0, 7, lambda i: first(pieces, pl.multiple_of(TOP + 8 + i * 16, 8), 16, closed))
        loop(0, 6, lambda i: second(results, 4 + i * 4, 16, part))

    def edge_rows(pieces, closed, results, part):
        first(pieces, TOP - 8, 8, closed, has_low)
        first(pieces, TOP + ROWS, 8, closed, has_high)
        loop(0, 2, lambda j: first(pieces, pl.multiple_of(TOP + j * (ROWS - 8), 8), 8, closed))
        loop(0, 2, lambda j: second(results, j * (NB - 4), 16, part))

    pair_a = halo(hal_a, msg_a, 0)
    pair_b = halo(hal_b, msg_b, 2)

    pass_on(pair_a, move_a)
    loop(NB - HOLD, NB, lambda k: move_b(neighbour(me, k), me).start())
    collect(move_a, msg_a, 0, EARLY)
    early, late = (0, 1), (2, 3)
    inner_rows((0, 1, 2), 2, early, part_a)
    halo_in(pair_a, hal_a, 0, EARLY)
    edge_rows((0, 1, 2), 2, early, part_a)

    plan_copy.wait()

    def fill2(out, part, d):
        out[d, 0] = part[plan_s[0, 2 * NB + d]]
        out[d, 1] = part[plan_s[0, 3 * NB + d]]

    loop(0, NB, lambda d: fill2(out_a, part_a, d))
    loop(1, NB - HOLD, lambda k: share_a(neighbour(me, k), me).start())
    own_a = pltpu.make_async_copy(out_a.at[me], arr_a.at[me], loc.at[2])
    own_a.start()

    pass_on(pair_b, move_b)
    loop(NB - HOLD, NB, lambda k: share_a(neighbour(me, k), me).start())
    collect(move_b, msg_b, EARLY, LATE)
    inner_rows((2, 3), None, late, part_b)
    halo_in(pair_b, hal_b, EARLY, LATE)
    edge_rows((2, 3), None, late, part_b)
    loop(0, NB, lambda d: fill2(out_b, part_b, d))
    loop(1, NB, lambda k: share_b(neighbour(me, k), me).start())
    own_b = pltpu.make_async_copy(out_b.at[me], arr_b.at[me], loc.at[3])
    own_b.start()
    vel_out = pltpu.make_async_copy(vel, vel_ref, loc.at[4])
    vel_out.start()

    def finish(k):
        d = neighbour(me, k)
        move_a(d, me).wait_send()
        move_b(d, me).wait_send()
        tell(d, me).wait_send()
        tell(d, d).wait_recv()
        share_a(d, me).wait_send()
        share_a(d, d).wait_recv()

    loop(1, NB, finish)

    @pl.when(has_high)
    def _():
        pair_a[0].wait_send()
        pair_b[0].wait_send()

    @pl.when(has_low)
    def _():
        pair_a[1].wait_send()
        pair_b[1].wait_send()

    own_plan.wait()
    own_a.wait()
    own_b.wait()
    vel_out.wait()

    def finish_b(k):
        d = neighbour(me, k)
        share_b(d, me).wait_send()
        share_b(d, d).wait_recv()

    loop(1, NB, finish_b)


def last_kernel(
    got_ref, arr_a, arr_b, vel_ref, mass_ref, heat_ref, velo_ref,
    got, arr, vel, acc, out, sem,
):
    me = lax.axis_index("bis")
    ins = [
        pltpu.make_async_copy(got_ref, got, sem.at[0]),
        pltpu.make_async_copy(arr_a, arr.at[0], sem.at[1]),
        pltpu.make_async_copy(arr_b, arr.at[1], sem.at[2]),
        pltpu.make_async_copy(vel_ref, vel, sem.at[3]),
    ]
    for copy in ins:
        copy.start()
    acc[...] = jnp.zeros(acc.shape, F32)
    ins[0].wait()
    outs = []
    for h in range(2):
        ins[1 + h].wait()

        def add(s, carry):
            for i in range(4):
                for k in range(2):
                    at = got[s * 4 + i, 0, k * NB + me]
                    acc[h, at] += arr[h, s * 4 + i, k]
            return carry

        lax.fori_loop(0, NB // 4, add, 0)
        if h == 0:
            ins[3].wait()
            outs.append(pltpu.make_async_copy(vel, velo_ref, sem.at[4]))
            outs[0].start()
        for q in range(2):
            for c in range(2):
                lanes = slice((h * 2 + c) * LANE, (h * 2 + c + 1) * LANE)
                for b in range(NB):
                    out[q, b * BR : b * BR + BR, lanes] = acc[
                        h, b, q * 8 + c * BR : q * 8 + c * BR + BR, :
                    ]
    for q, ref in enumerate((mass_ref, heat_ref)):
        outs.append(pltpu.make_async_copy(out.at[q], ref, sem.at[5 + q]))
        outs[-1].start()
    for copy in outs:
        copy.wait()


def shards(state, order, sweep, owner, slot_target):
    any_ = pl.BlockSpec(memory_space=pl.ANY)
    vmem = pl.BlockSpec(memory_space=pltpu.VMEM)
    smem = pl.BlockSpec(memory_space=pltpu.SMEM)
    dma = pltpu.SemaphoreType.DMA
    half = jax.ShapeDtypeStruct((NB, 2, 16, LANE), F32)
    arr_a, arr_b, got, vel = pl.pallas_call(
        main_kernel,
        name="step",
        out_shape=(
            half,
            half,
            jax.ShapeDtypeStruct((NB, 1, LANE), jnp.int32),
            jax.ShapeDtypeStruct((2, ROWS, W), F32),
        ),
        in_specs=[smem, vmem, vmem, any_, vmem],
        out_specs=(any_, any_, any_, any_),
        scratch_shapes=[
            pltpu.VMEM((5, ROWS, W), F32),
            pltpu.VMEM((NB, 5, EARLY, BR, LANE), F32),
            pltpu.VMEM((NB, 5, LATE, BR, LANE), F32),
            pltpu.VMEM((NB, 5, EARLY, BR, LANE), F32),
            pltpu.VMEM((NB, 5, LATE, BR, LANE), F32),
            pltpu.VMEM((NB, 5, EARLY, BR, LANE), F32),
            pltpu.VMEM((NB, 5, LATE, BR, LANE), F32),
            pltpu.VMEM((2, 5, EARLY, BR, LANE), F32),
            pltpu.VMEM((2, 5, LATE, BR, LANE), F32),
            pltpu.VMEM((5, PIECES, EXT, LANE), F32),
            pltpu.VMEM((5, PIECES, EXT, LANE), F32),
            pltpu.VMEM((PIECES, EXT, LANE), F32),
            pltpu.VMEM((PIECES, EXT, LANE), F32),
            pltpu.VMEM((NB, 16, LANE), F32),
            pltpu.VMEM((NB, 16, LANE), F32),
            pltpu.VMEM((NB, 2, 16, LANE), F32),
            pltpu.VMEM((NB, 2, 16, LANE), F32),
            pltpu.VMEM((2, ROWS, W), F32),
            pltpu.VMEM((1, LANE), jnp.int32),
            pltpu.SMEM((1, LANE), jnp.int32),
            dma((5,)),
            dma((NB,)), dma((NB,)), dma((NB,)), dma((NB,)),
            dma((NB,)), dma((NB,)),
            dma((4,)), dma((4,)),
            dma((NB,)), dma((NB,)), dma((NB,)), dma((NB,)),
            dma((5,)),
        ],
        compiler_params=pltpu.CompilerParams(collective_id=0, has_side_effects=True),
    )(order, owner.reshape(1, NB), slot_target.reshape(1, NB), state, sweep)
    field = jax.ShapeDtypeStruct((ROWS, W), F32)
    return pl.pallas_call(
        last_kernel,
        name="gather",
        out_shape=(field, field, jax.ShapeDtypeStruct((2, ROWS, W), F32)),
        in_specs=[any_, any_, any_, any_],
        out_specs=(any_, any_, any_),
        scratch_shapes=[
            pltpu.SMEM((NB, 1, LANE), jnp.int32),
            pltpu.VMEM((2, NB, 2, 16, LANE), F32),
            pltpu.VMEM((2, ROWS, W), F32),
            pltpu.VMEM((2, NB + 1, 16, LANE), F32),
            pltpu.VMEM((2, ROWS, W), F32),
            dma((7,)),
        ],
    )(got, arr_a, arr_b, vel)


def solution(mesh):
    rows = P(("grp", "bis"), None)
    return jax.shard_map(
        shards,
        mesh=mesh,
        in_specs=(P(None, ("grp", "bis"), None), rows, rows, rows, P(("grp", "bis"))),
        out_specs=(rows, rows, P(None, ("grp", "bis"), None)),
        check_vma=False,
    )
```

```python
import jax
import jax.numpy as jnp
from jax import lax
from jax.experimental import pallas as pl
from jax.experimental.pallas import tpu as pltpu
from jax.sharding import PartitionSpec as P

DT = 0.15
NB = 32
NG = 8
W = 512
ROWS = 128
BR = 4
LANE = 128
PIECES = W // LANE
EARLY = 3
LATE = PIECES - EARLY
TOP = 16
EXT = TOP + ROWS + 16
MESH = pl.DeviceIdType.MESH
STRIDE = 9
HALF = BR // 2
PAIRS = NB // 2
F32 = jnp.float32


ORDER = [(j // 8, j // 2 % 4, j % 2) for j in (k * STRIDE % NB for k in range(1, NB))]


def lane_mask(size, lane):
    return lax.broadcasted_iota(jnp.int32, (size, LANE), 1) == lane


def advance(piece, at, size, fields, press, closed):
    def ld(ref, off=0, where=piece):
        return ref[where, pl.ds(at + off, size), :]

    def columns(ref):
        here = ld(ref)
        before = ld(ref, 0, piece - 1) if piece > 0 else 0.0
        after = ld(ref, 0, piece + 1) if piece + 1 < PIECES and not closed else 0.0
        left = pltpu.roll(jnp.where(lane_mask(size, LANE - 1), before, here), 1, 1)
        right = pltpu.roll(jnp.where(lane_mask(size, 0), after, here), LANE - 1, 1)
        return right - left

    rho, ene, velu, velv, gam = fields
    dens = ld(rho)
    grad_x = 0.5 * (ld(press, 1) - ld(press, -1))
    grad_y = 0.5 * columns(press)
    spread = 0.5 * (ld(velu, 1) - ld(velu, -1) + columns(velv))
    growth = 1.0 + DT * spread
    inverse = 1.0 / dens
    gamma = ld(gam)
    return (
        dens / growth,
        ld(ene) * (1.0 - DT * (gamma - 1.0) * spread),
        ld(velu) - DT * grad_x * inverse,
        ld(velv) - DT * grad_y * inverse,
        growth,
        gamma,
    )


def main_kernel(
    order_ref, owner_ref, slot_ref, state_ref, sweep_ref,
    arr_a, arr_b, got_ref, vel_ref,
    xv, lin_a, lin_b, snd_a, snd_b, msg_a, msg_b, dir_a, dir_b, hal_a, hal_b, fwd_a, fwd_b,
    ext, one, press0, press1, part_a, part_b, out_a, out_b, vel, plan_v, plan_s,
    in_sem, s1a, r1a, s1b, r1b, sm, rm, sd, sh, rh, s2a, r2a, s2b, r2b, loc,
):
    grp = lax.axis_index("grp")
    me = lax.axis_index("bis")
    whole = grp * NB + me
    has_low = whole > 0
    has_high = whole < NG * NB - 1
    first_one = me == 0
    last_one = me == NB - 1
    low = (grp - first_one.astype(jnp.int32), lax.rem(me + NB - 1, NB))
    high = (grp + last_one.astype(jnp.int32), lax.rem(me + 1, NB))
    odd = lax.rem(me, 2)
    at_x = [lax.rem(me // 8 + d, 4) * 8 for d in range(4)]
    at_y = [lax.rem(me // 2 + d, 4) * 2 for d in range(4)]
    at_c = [odd, 1 - odd]
    peers = [at_x[dx] + at_y[dy] + at_c[dc] for dx, dy, dc in ORDER]
    odd_not = 1 - odd
    partner = me + 1 - 2 * odd
    inside = (NB - 1) * odd_not
    has_direct = jnp.where(odd == 0, has_low, has_high)
    sends_direct = jnp.logical_or(first_one, last_one)
    begin = jnp.logical_and(first_one, grp == 0).astype(jnp.int32)
    end = PAIRS - jnp.logical_and(last_one, grp == NG - 1).astype(jnp.int32)
    far_low = jnp.logical_and(first_one, has_low)
    far_high = jnp.logical_and(last_one, has_high)

    loads = [pltpu.make_async_copy(state_ref.at[f], xv.at[f], in_sem.at[f]) for f in range(5)]
    for load in loads:
        load.start()

    barrier = pltpu.get_barrier_semaphore()

    def loop(lo, hi, body, unroll=1):
        def step(k, carry):
            body(k)
            return carry

        lax.fori_loop(lo, hi, step, 0, unroll=unroll)

    def others(body):
        def step(d, carry):
            @pl.when(d != me)
            def _():
                body(d)

            return carry

        lax.fori_loop(0, NB, step, 0)

    others(
        lambda d: pl.semaphore_signal(
            barrier, inc=1, device_id=(grp, d), device_id_type=MESH
        )
    )

    @pl.when(far_low)
    def _():
        pl.semaphore_signal(barrier, inc=1, device_id=low, device_id_type=MESH)

    @pl.when(far_high)
    def _():
        pl.semaphore_signal(barrier, inc=1, device_id=high, device_id_type=MESH)

    row = lax.broadcasted_iota(jnp.int32, (NB, LANE), 0)
    lane = lax.broadcasted_iota(jnp.int32, (NB, LANE), 1)
    same = lax.broadcasted_iota(jnp.int32, (NB, NB), 0) == lax.broadcasted_iota(
        jnp.int32, (NB, NB), 1
    )

    def column(ref):
        spread = jnp.where(same, jnp.broadcast_to(ref[...], (NB, NB)), 0)
        return jnp.sum(spread, axis=1, keepdims=True)

    code = row * NB + column(slot_ref)
    hit = jnp.broadcast_to(column(owner_ref), (NB, LANE)) == lax.rem(lane, NB)
    least = jnp.min(jnp.where(hit, code, NB * NB), axis=0, keepdims=True)
    most = jnp.max(jnp.where(hit, code, -1), axis=0, keepdims=True)
    at_lane = lax.broadcasted_iota(jnp.int32, (1, LANE), 1)
    plan_v[...] = jnp.where(
        at_lane < NB,
        jnp.where(least < NB * NB, least & (NB - 1), NB),
        jnp.where(
            at_lane < 2 * NB,
            jnp.where(most > least, most & (NB - 1), NB),
            jnp.where(
                at_lane < 3 * NB,
                jnp.minimum(least >> 5, NB - 1),
                jnp.maximum(most, 0) >> 5,
            ),
        ),
    )

    for f in range(5):
        loads[f].wait()
        for c in range(PIECES):
            for b in range(NB):
                half = xv[f, b * BR : b * BR + BR, c * LANE : c * LANE + LANE]
                if c < EARLY:
                    lin_a[b, f, c] = half
                else:
                    lin_b[b, f, c - EARLY] = half

    plan_copy = pltpu.make_async_copy(plan_v, plan_s, loc.at[0])
    plan_copy.start()
    pl.semaphore_wait(
        barrier, NB - 1 + far_low.astype(jnp.int32) + far_high.astype(jnp.int32)
    )

    def remote(src, dst, send, recv, d):
        return pltpu.make_async_remote_copy(
            src_ref=src, dst_ref=dst, send_sem=send, recv_sem=recv,
            device_id=(grp, d), device_id_type=MESH,
        )

    def move_a(d, source):
        return remote(snd_a.at[d], msg_a.at[source], s1a.at[d], r1a.at[source], d)

    def move_b(d, source):
        return remote(snd_b.at[d], msg_b.at[source], s1b.at[d], r1b.at[source], d)

    def tell(d, source):
        return remote(plan_v, got_ref.at[source], sm.at[d], rm.at[source], d)

    def share_a(d, source):
        return remote(out_a.at[d], arr_a.at[source], s2a.at[d], r2a.at[source], d)

    def share_b(d, source):
        return remote(out_b.at[d], arr_b.at[source], s2b.at[d], r2b.at[source], d)

    def direct_one(dire, hal, j, at):
        index = 2 * j + 3 * odd - 1
        step = (index + NB) // NB - 1
        return pltpu.make_async_remote_copy(
            src_ref=dire.at[j], dst_ref=hal, send_sem=sd.at[at, j], recv_sem=rh.at[2 + at],
            device_id=(grp + step, index - step * NB), device_id_type=MESH,
        )

    def direct(dire, hal, lin, at):
        @pl.when(first_one)
        def _():
            def pack(j):
                dire[j] = lin[order_ref[0, 2 * j], :, :, 0:HALF]

            loop(begin, end, pack)

        @pl.when(last_one)
        def _():
            def pack(j):
                dire[j] = lin[order_ref[0, 2 * j + 1], :, :, HALF:BR]

            loop(begin, end, pack)

        @pl.when(sends_direct)
        def _():
            loop(begin, end, lambda j: direct_one(dire, hal, j, at).start())

    def fill_a(d):
        snd_a[d] = lin_a[order_ref[0, d]]

    def fill_b(d):
        snd_b[d] = lin_b[order_ref[0, d]]

    def rounds(fill, send):
        fill(peers[0])
        for k, d in enumerate(peers):
            if k + 1 < len(peers):
                fill(peers[k + 1])
            send(d, me).start()

    rounds(fill_a, move_a)
    direct(dir_a, hal_a, lin_a, 0)
    rounds(fill_b, move_b)
    direct(dir_b, hal_b, lin_b, 1)
    others(lambda d: tell(d, me).start())
    own_plan = pltpu.make_async_copy(plan_v, got_ref.at[me], loc.at[1])
    own_plan.start()
    msg_a[me] = lin_a[order_ref[0, me]]
    msg_b[me] = lin_b[order_ref[0, me]]

    zero = jnp.zeros((TOP, LANE), F32)
    for c in range(PIECES):
        for f in range(5):
            ext[f, c, 0:TOP, :] = zero
            ext[f, c, EXT - 16 : EXT, :] = zero
        press0[c, 0:TOP, :] = zero
        press0[c, EXT - 16 : EXT, :] = zero

    def spread_out(values, c, at, size=BR):
        for f in range(5):
            ext[f, c, pl.ds(at, size), :] = values[f]
        press0[c, pl.ds(at, size), :] = (values[4] - 1.0) * values[0] * values[1]

    def unpack(msg, base, count, source):
        for c in range(count):
            spread_out([msg[source, f, c] for f in range(5)], base + c, TOP + source * BR)

    def forward(msg, fwd, at):
        return remote(msg.at[inside], fwd, sh.at[at], rh.at[at], partner)

    def pass_on(msg, fwd, move, at):
        move(inside, inside).wait_recv()
        forward(msg, fwd, at).start()

    def collect(move, msg, base, count):
        def one_source(source):
            @pl.when(jnp.logical_and(source != inside, source != me))
            def _():
                move(source, source).wait_recv()

            unpack(msg, base, count, source)

        loop(0, NB, one_source)

    def halo_in(dire, hal, msg, fwd, base, count, at):
        forward(msg, fwd, at).wait_recv()
        beside = TOP - BR + odd_not * (ROWS + BR)
        for c in range(count):
            spread_out([fwd[f, c] for f in range(5)], base + c, beside)

        @pl.when(has_direct)
        def _():
            direct_one(dire, hal, 0, at).wait_recv()
            across = TOP - HALF + odd * (ROWS + HALF)
            for c in range(count):
                spread_out([hal[f, c] for f in range(5)], base + c, across, HALF)

    start = [ext.at[f] for f in range(5)]
    after = [one.at[f] for f in range(4)] + [ext.at[4]]

    def first(pieces, at, size, closed=None, keep=None):
        rows = pl.ds(at, size)
        done = [advance(c, at, size, start, press0, c == closed) for c in pieces]
        for c, (rho, ene, velu, velv, growth, gamma) in zip(pieces, done):
            pre = (gamma - 1.0) * rho * ene
            if keep is not None:
                velu = jnp.where(keep, velu, 0.0)
                pre = jnp.where(keep, pre, 0.0)
            one[0, c, rows, :] = rho
            one[1, c, rows, :] = ene
            one[2, c, rows, :] = velu
            one[3, c, rows, :] = velv
            one[4, c, rows, :] = growth
            press1[c, rows, :] = pre

    def second(pieces, block, size, part):
        mesh_row = pl.multiple_of(block * BR, 8)
        at = pl.multiple_of(TOP + block * BR, 8)
        done = [advance(c, at, size, after, press1, False) for c in pieces]
        head = lax.rem(lax.broadcasted_iota(jnp.int32, (size, LANE), 0), BR) == 0

        def mixed(value, frac):
            away = frac * value
            near = pltpu.roll(away, 1, 0)
            wrap = pltpu.roll(away, size - (BR - 1), 0)
            return (1.0 - frac) * value + jnp.where(head, wrap, near)

        for c, (rho, ene, velu, velv, growth, _) in zip(pieces, done):
            columns = slice(c * LANE, c * LANE + LANE)
            volume = one[4, c, pl.ds(at, size), :] * growth
            vel[0, pl.ds(mesh_row, size), columns] = velu
            vel[1, pl.ds(mesh_row, size), columns] = velv
            mass = rho * volume
            heat = mass * ene
            frac = sweep_ref[pl.ds(mesh_row, size), columns] * volume / (1.0 + volume)
            for q, value in enumerate((mixed(mass, frac), mixed(heat, frac))):
                put = q * 8 + (c % 2) * BR
                for i in range(size // BR):
                    part[block + i, put : put + BR, :] = value[i * BR : i * BR + BR]

    def inner_rows(pieces, closed, results, part):
        loop(0, 7, lambda i: first(pieces, pl.multiple_of(TOP + 8 + i * 16, 8), 16, closed), 7)
        loop(0, 6, lambda i: second(results, 4 + i * 4, 16, part), 3)

    def edge_rows(pieces, closed, results, part):
        first(pieces, TOP - 8, 8, closed, has_low)
        first(pieces, TOP + ROWS, 8, closed, has_high)
        loop(0, 2, lambda j: first(pieces, pl.multiple_of(TOP + j * (ROWS - 8), 8), 8, closed))
        loop(0, 2, lambda j: second(results, j * (NB - 4), 16, part))

    pass_on(msg_a, fwd_a, move_a, 0)
    collect(move_a, msg_a, 0, EARLY)
    early, late = (0, 1), (2, 3)
    inner_rows((0, 1, 2), 2, early, part_a)
    halo_in(dir_a, hal_a, msg_a, fwd_a, 0, EARLY, 0)
    edge_rows((0, 1, 2), 2, early, part_a)

    plan_copy.wait()

    def fill2(out, part, d):
        out[d, 0] = part[plan_s[0, 2 * NB + d]]
        out[d, 1] = part[plan_s[0, 3 * NB + d]]

    rounds(lambda d: fill2(out_a, part_a, d), share_a)
    fill2(out_a, part_a, me)
    own_a = pltpu.make_async_copy(out_a.at[me], arr_a.at[me], loc.at[2])
    own_a.start()

    pass_on(msg_b, fwd_b, move_b, 1)
    collect(move_b, msg_b, EARLY, LATE)
    inner_rows((2, 3), None, late, part_b)
    halo_in(dir_b, hal_b, msg_b, fwd_b, EARLY, LATE, 1)
    edge_rows((2, 3), None, late, part_b)
    rounds(lambda d: fill2(out_b, part_b, d), share_b)
    fill2(out_b, part_b, me)
    own_b = pltpu.make_async_copy(out_b.at[me], arr_b.at[me], loc.at[3])
    own_b.start()
    vel_out = pltpu.make_async_copy(vel, vel_ref, loc.at[4])
    vel_out.start()

    def finish(d):
        move_a(d, me).wait_send()
        move_b(d, me).wait_send()
        tell(d, me).wait_send()
        tell(d, d).wait_recv()
        share_a(d, me).wait_send()
        share_a(d, d).wait_recv()

    others(finish)

    forward(msg_a, fwd_a, 0).wait_send()
    forward(msg_b, fwd_b, 1).wait_send()

    @pl.when(sends_direct)
    def _():
        for at, (dire, hal) in enumerate(((dir_a, hal_a), (dir_b, hal_b))):
            loop(begin, end, lambda j, a=(dire, hal), at=at: direct_one(*a, j, at).wait_send())

    own_plan.wait()
    own_a.wait()
    own_b.wait()
    vel_out.wait()

    def finish_b(d):
        share_b(d, me).wait_send()
        share_b(d, d).wait_recv()

    others(finish_b)


def last_kernel(
    got_ref, arr_a, arr_b, vel_ref, mass_ref, heat_ref, velo_ref,
    got, arr, vel, acc, out, sem,
):
    me = lax.axis_index("bis")
    ins = [
        pltpu.make_async_copy(got_ref, got, sem.at[0]),
        pltpu.make_async_copy(arr_a, arr.at[0], sem.at[1]),
        pltpu.make_async_copy(arr_b, arr.at[1], sem.at[2]),
        pltpu.make_async_copy(vel_ref, vel, sem.at[3]),
    ]
    for copy in ins:
        copy.start()
    acc[...] = jnp.zeros(acc.shape, F32)
    ins[0].wait()
    outs = []
    for h in range(2):
        ins[1 + h].wait()

        def add(s, carry):
            for i in range(4):
                for k in range(2):
                    at = got[s * 4 + i, 0, k * NB + me]
                    acc[h, at] += arr[h, s * 4 + i, k]
            return carry

        lax.fori_loop(0, NB // 4, add, 0)
        if h == 0:
            ins[3].wait()
            outs.append(pltpu.make_async_copy(vel, velo_ref, sem.at[4]))
            outs[0].start()
        for q in range(2):
            for c in range(2):
                lanes = slice((h * 2 + c) * LANE, (h * 2 + c + 1) * LANE)
                for b in range(NB):
                    out[q, b * BR : b * BR + BR, lanes] = acc[
                        h, b, q * 8 + c * BR : q * 8 + c * BR + BR, :
                    ]
    for q, ref in enumerate((mass_ref, heat_ref)):
        outs.append(pltpu.make_async_copy(out.at[q], ref, sem.at[5 + q]))
        outs[-1].start()
    for copy in outs:
        copy.wait()


def shards(state, order, sweep, owner, slot_target):
    any_ = pl.BlockSpec(memory_space=pl.ANY)
    vmem = pl.BlockSpec(memory_space=pltpu.VMEM)
    smem = pl.BlockSpec(memory_space=pltpu.SMEM)
    dma = pltpu.SemaphoreType.DMA
    half = jax.ShapeDtypeStruct((NB, 2, 16, LANE), F32)
    arr_a, arr_b, got, vel = pl.pallas_call(
        main_kernel,
        name="step",
        out_shape=(
            half,
            half,
            jax.ShapeDtypeStruct((NB, 1, LANE), jnp.int32),
            jax.ShapeDtypeStruct((2, ROWS, W), F32),
        ),
        in_specs=[smem, vmem, vmem, any_, vmem],
        out_specs=(any_, any_, any_, any_),
        scratch_shapes=[
            pltpu.VMEM((5, ROWS, W), F32),
            pltpu.VMEM((NB, 5, EARLY, BR, LANE), F32),
            pltpu.VMEM((NB, 5, LATE, BR, LANE), F32),
            pltpu.VMEM((NB, 5, EARLY, BR, LANE), F32),
            pltpu.VMEM((NB, 5, LATE, BR, LANE), F32),
            pltpu.VMEM((NB, 5, EARLY, BR, LANE), F32),
            pltpu.VMEM((NB, 5, LATE, BR, LANE), F32),
            pltpu.VMEM((PAIRS, 5, EARLY, HALF, LANE), F32),
            pltpu.VMEM((PAIRS, 5, LATE, HALF, LANE), F32),
            pltpu.VMEM((5, EARLY, HALF, LANE), F32),
            pltpu.VMEM((5, LATE, HALF, LANE), F32),
            pltpu.VMEM((5, EARLY, BR, LANE), F32),
            pltpu.VMEM((5, LATE, BR, LANE), F32),
            pltpu.VMEM((5, PIECES, EXT, LANE), F32),
            pltpu.VMEM((5, PIECES, EXT, LANE), F32),
            pltpu.VMEM((PIECES, EXT, LANE), F32),
            pltpu.VMEM((PIECES, EXT, LANE), F32),
            pltpu.VMEM((NB, 16, LANE), F32),
            pltpu.VMEM((NB, 16, LANE), F32),
            pltpu.VMEM((NB, 2, 16, LANE), F32),
            pltpu.VMEM((NB, 2, 16, LANE), F32),
            pltpu.VMEM((2, ROWS, W), F32),
            pltpu.VMEM((1, LANE), jnp.int32),
            pltpu.SMEM((1, LANE), jnp.int32),
            dma((5,)),
            dma((NB,)), dma((NB,)), dma((NB,)), dma((NB,)),
            dma((NB,)), dma((NB,)),
            dma((2, PAIRS)), dma((2,)), dma((4,)),
            dma((NB,)), dma((NB,)), dma((NB,)), dma((NB,)),
            dma((5,)),
        ],
        compiler_params=pltpu.CompilerParams(collective_id=0, has_side_effects=True),
    )(order, owner.reshape(1, NB), slot_target.reshape(1, NB), state, sweep)
    field = jax.ShapeDtypeStruct((ROWS, W), F32)
    return pl.pallas_call(
        last_kernel,
        name="gather",
        out_shape=(field, field, jax.ShapeDtypeStruct((2, ROWS, W), F32)),
        in_specs=[any_, any_, any_, any_],
        out_specs=(any_, any_, any_),
        scratch_shapes=[
            pltpu.SMEM((NB, 1, LANE), jnp.int32),
            pltpu.VMEM((2, NB, 2, 16, LANE), F32),
            pltpu.VMEM((2, ROWS, W), F32),
            pltpu.VMEM((2, NB + 1, 16, LANE), F32),
            pltpu.VMEM((2, ROWS, W), F32),
            dma((7,)),
        ],
    )(got, arr_a, arr_b, vel)


def solution(mesh):
    rows = P(("grp", "bis"), None)
    return jax.shard_map(
        shards,
        mesh=mesh,
        in_specs=(P(None, ("grp", "bis"), None), rows, rows, rows, P(("grp", "bis"))),
        out_specs=(rows, rows, P(None, ("grp", "bis"), None)),
        check_vma=False,
    )
```
